32 devices in a mesh: node: 4 (over y, x), torus: 8 (over z, core).
Axes of the slice: x: 2, y: 2, z: 4, core: 2. Of those that a mesh axis runs over, the one named last changes fastest.
Arguments:
- tokens: bfloat16 [4096, 7168], P(('node', 'torus')), may hold values from -6 to 6
- expert_ids: int32 [4096, 8], P(('node', 'torus')), may hold values from 0 to 383, as said below
- route_weight: bfloat16 [4096, 8], P(('node', 'torus')), may hold values from 0.19921875 to 2.5
- w_gate: bfloat16 [16, 7168, 1024], P('torus', None, 'node'), may hold values from -0.0625 to 0.0625
- w_up: bfloat16 [16, 7168, 1024], P('torus', None, 'node'), may hold values from -0.0625 to 0.0625
- w_down: bfloat16 [16, 1024, 7168], P('torus', 'node'), may hold values from -0.1875 to 0.1875
Outputs:
- moe_out: bfloat16 [4096, 7168], P(('node', 'torus'))
The draws below stay inside these ranges and needn't reach their ends.
Inputs may be any that keep to these rules, and one draw needn't show every extreme that they name: `expert_ids`: each row names 8 different experts. Counting an expert e below 16 as one of group e // 2, at most 4 of the 128 rows of one device (aligned blocks of rows, in order) name an expert of any one group, and in every draw some group is named by exactly 4 rows of every device.
All inputs are finite; a program needn't handle non-finite values.
Results may differ from the reference program's by a relative error of at most 0.0095.
Values may be sent and summed in bfloat16 or wider, within the bound.
No kernel may reach another device: no remote copies, remote signals or barrier semaphores. Data moves between devices by JAX's collectives and lax.ppermute only.
A program may use at most 128 MiB of HBM per device.

```python
import math
import jax
import jax.numpy as jnp
from jax import lax

D = 7168
FF = 1024
EXPERTS = 384
TOPK = 8
EXP_DEV = 2
CAP = 4
QBLOCK = 128
TOK_DEV = 128
GROUPS = 8
SOURCES = 32
WIN_EXPERTS = 16
TOKENS = 4096
N_NODE = 4


def draw_expert_ids(key, part):
    keys = jax.random.split(jax.random.fold_in(key, 17), 8)
    group_ids = jnp.arange(GROUPS, dtype=jnp.int32)
    hot_group = jax.random.randint(keys[0], (), 0, GROUPS, dtype=jnp.int32)
    second_group = jax.random.randint(keys[1], (SOURCES,), 0, GROUPS, dtype=jnp.int32)
    second_used = jax.random.randint(keys[2], (SOURCES,), 0, 2, dtype=jnp.int32)
    counts = jax.random.randint(keys[3], (SOURCES, GROUPS), 1, 4, dtype=jnp.int32)
    counts = jnp.where(group_ids[None, :] == hot_group, CAP, counts)
    counts = jnp.where((group_ids[None, :] == second_group[:, None]) & (second_used[:, None] == 1), CAP, counts)
    ends = jnp.cumsum(counts, axis=1).astype(jnp.int32)
    laps = TOPK // EXP_DEV
    position = jnp.arange(laps * TOK_DEV, dtype=jnp.int32).reshape(laps, TOK_DEV)
    owner = jnp.sum((ends[:, None, None, :] <= position[None, :, :, None]).astype(jnp.int32), axis=-1)
    inside = position[None, :, :] < ends[:, -1][:, None, None]
    picked = jax.random.randint(keys[4], (SOURCES, laps, TOK_DEV), 0, 3, dtype=jnp.int32)
    first = EXP_DEV * owner + (picked == 1).astype(jnp.int32)
    second = EXP_DEV * owner + 1
    first = jnp.where(inside, first, -1)
    second = jnp.where(inside & (picked == 2), second, -1)
    paired = jnp.stack([first, second], axis=2)
    slots = paired.reshape(SOURCES, TOPK, TOK_DEV).transpose(0, 2, 1)
    shuffles = jax.vmap(lambda sub: jax.random.permutation(sub, TOK_DEV))(jax.random.split(keys[5], SOURCES))
    inverse = jnp.argsort(shuffles, axis=1).astype(jnp.int32)
    slots = jnp.take_along_axis(slots, inverse[:, :, None], axis=1)
    remain = EXPERTS - WIN_EXPERTS
    offset = jax.random.randint(keys[6], (SOURCES, TOK_DEV, 1), 0, remain, dtype=jnp.int32)
    filler = WIN_EXPERTS + (offset + jnp.arange(TOPK, dtype=jnp.int32)[None, None, :]) % remain
    chosen = jnp.where(slots >= 0, slots, filler)
    scores = jax.random.randint(keys[7], (SOURCES, TOK_DEV, TOPK), 0, 1 << 20, dtype=jnp.int32) * TOPK + jnp.arange(TOPK, dtype=jnp.int32)[None, None, :]
    order = jnp.argsort(scores, axis=-1, stable=True)
    chosen = jnp.take_along_axis(chosen, order, axis=-1)
    return chosen.reshape(TOKENS, TOPK).astype(jnp.int32)


def steps_of(stream_key, dims, cuts, least, high):
    gain, own = 1.0, jax.random.fold_in(stream_key, 6)
    for axis_at, shards_of in cuts:
        draws = jnp.exp(jax.random.uniform(jax.random.fold_in(own, axis_at), (shards_of,), jnp.float32, least / len(cuts), high / len(cuts)))
        gain = gain * jnp.repeat(draws, dims[axis_at] // shards_of).reshape([-1 if axis == axis_at else 1 for axis in range(len(dims))])
    return gain


def centred(stream_key, shape, width, bound, cuts=(), held_as=jnp.bfloat16):
    loudness = steps_of(stream_key, shape, cuts, -0.22, 0.18) if cuts else 1.0
    drawn = jax.random.normal(stream_key, shape, jnp.float32) * width * loudness
    return jnp.minimum(jnp.maximum(drawn, -bound), bound).astype(held_as)


def setup_inputs(seed: int = 0) -> dict:
    streams_of = jax.random.split(jax.random.key(seed), 7)
    tokens = centred(streams_of[0], (TOKENS, D), 1.0, 6.0, ((0, 32),))
    expert_ids = draw_expert_ids(jax.random.fold_in(streams_of[6], 71), 0)
    route_weight = jnp.clip(jnp.exp(math.log(2.5) - 2.5296425 * jax.random.uniform(streams_of[2], (TOKENS, TOPK), jnp.float32) ** steps_of(streams_of[2], (TOKENS, TOPK), ((0, 32),), -0.2, 0.2)), 0.19921875, 2.5).astype(jnp.bfloat16)
    w_gate = centred(streams_of[3], (WIN_EXPERTS, D, FF), D ** -0.5, 0.0625, ((0, 8), (2, 4)))
    w_up = centred(streams_of[4], (WIN_EXPERTS, D, FF), D ** -0.5, 0.0625, ((0, 8), (2, 4)))
    w_down = centred(streams_of[5], (WIN_EXPERTS, FF, D), FF ** -0.5, 0.1875, ((0, 8), (1, 4)))
    return {"tokens": tokens, "expert_ids": expert_ids, "route_weight": route_weight, "w_gate": w_gate, "w_up": w_up, "w_down": w_down}


block_rows = 64


def quantize(tokens):
    count = tokens.shape[0]
    blocks = tokens.astype(jnp.float32).reshape(count, -1, QBLOCK)
    largest = jnp.max(jnp.abs(blocks), axis=-1)
    scale = ((largest + 1e-6) * (1.0 / 448.0)).astype(jnp.bfloat16)
    scale = lax.optimization_barrier(scale)
    quantized = (blocks / scale.astype(jnp.float32)[:, :, None]).astype(jnp.bfloat16)
    quantized = lax.optimization_barrier(quantized)
    return quantized.reshape(count, -1), scale


def restore(quantized, scale):
    count = quantized.shape[0]
    blocks = quantized.astype(jnp.float32).reshape(count, -1, QBLOCK) * scale.astype(jnp.float32)[:, :, None]
    return blocks.astype(jnp.bfloat16).reshape(count, -1)


def reference(tokens, expert_ids, route_weight, w_gate, w_up, w_down):
    quantized, scale = quantize(tokens)
    restored = restore(quantized, scale)
    experts = jnp.arange(WIN_EXPERTS, dtype=jnp.int32)
    weight_float = route_weight.astype(jnp.float32)
    route_sel = jnp.zeros((TOKENS, WIN_EXPERTS), jnp.float32)
    named = jnp.zeros((TOKENS, WIN_EXPERTS), jnp.int32)
    for slot in range(TOPK):
        matched = expert_ids[:, slot:slot + 1] == experts[None, :]
        route_sel = route_sel + jnp.where(matched, weight_float[:, slot:slot + 1], jnp.float32(0.0))
        named = named + matched.astype(jnp.int32)
    member = named.reshape(TOKENS, GROUPS, EXP_DEV).sum(axis=-1)
    route_sel = route_sel.reshape(TOKENS, GROUPS, EXP_DEV)
    quarter = FF // N_NODE
    total = jnp.zeros((TOKENS, D), jnp.float32)
    offsets = jnp.arange(block_rows, dtype=jnp.int32)

    def group_step(group, total):
        inside = lax.dynamic_index_in_dim(member, group, 1, keepdims=False) > 0
        count = jnp.sum(inside.astype(jnp.int32)).astype(jnp.int32)
        order = jnp.argsort(jnp.where(inside, 0, 1).astype(jnp.int32), stable=True).astype(jnp.int32)
        order = jnp.concatenate([order, jnp.zeros((block_rows,), jnp.int32)])
        weights_group = lax.dynamic_index_in_dim(route_sel, group, 1, keepdims=False)
        gates = [lax.dynamic_index_in_dim(w_gate, EXP_DEV * group + expert, 0, keepdims=False) for expert in range(EXP_DEV)]
        ups = [lax.dynamic_index_in_dim(w_up, EXP_DEV * group + expert, 0, keepdims=False) for expert in range(EXP_DEV)]
        downs = [lax.dynamic_index_in_dim(w_down, EXP_DEV * group + expert, 0, keepdims=False) for expert in range(EXP_DEV)]

        def block_step(block, total):
            start = (block * block_rows).astype(jnp.int32)
            picked = lax.dynamic_slice_in_dim(order, start, block_rows)
            valid = (start + offsets) < count
            rows = restored[picked]
            weights = weights_group[picked]
            parts = [jnp.zeros((block_rows, D), jnp.float32) for piece in range(N_NODE)]
            for expert in range(EXP_DEV):
                gate = jnp.dot(rows, gates[expert], preferred_element_type=jnp.float32)
                upper = jnp.dot(rows, ups[expert], preferred_element_type=jnp.float32)
                hidden = (jax.nn.silu(gate) * upper).astype(jnp.bfloat16)
                for piece in range(N_NODE):
                    lower = piece * quarter
                    result = jnp.dot(hidden[:, lower:lower + quarter], downs[expert][lower:lower + quarter, :], preferred_element_type=jnp.float32)
                    parts[piece] = parts[piece] + weights[:, expert:expert + 1] * result
            combined = jnp.zeros((block_rows, D), jnp.float32)
            for piece in range(N_NODE):
                rounded = lax.optimization_barrier(parts[piece].astype(jnp.bfloat16))
                combined = combined + rounded.astype(jnp.float32)
            combined = lax.optimization_barrier(combined.astype(jnp.bfloat16))
            added = jnp.where(valid[:, None], combined.astype(jnp.float32), jnp.float32(0.0))
            return total.at[picked].add(added)

        blocks = (count + block_rows - 1) // block_rows
        return lax.fori_loop(0, blocks, block_step, total)

    total = lax.fori_loop(0, GROUPS, group_step, total)
    return total.astype(jnp.bfloat16)
```

```python
import functools

import jax
import jax.numpy as jnp
from jax import lax
from jax.experimental import pallas as pl
from jax.experimental.pallas import tpu as pltpu
from jax.sharding import PartitionSpec as P

EXP_DEV = 2
CAP = 4
QBLOCK = 128
PAIR = 2
UNIT = PAIR * CAP
LANES = 128


VMEM = pl.BlockSpec(memory_space=pltpu.VMEM)
SMEM = pl.BlockSpec(memory_space=pltpu.SMEM)


def pack_kernel(hops, step, where_ref, ids_ref, route_ref, tokens_ref, keep_ref, give_ref, place_ref):
    count, width = tokens_ref.shape
    names = ids_ref.shape[0]
    rows = 2 * hops * UNIT
    line, core = where_ref[0], where_ref[1]
    row = lax.broadcasted_iota(jnp.int32, (rows, count), 0)
    half = row // (hops * UNIT)
    hop = (row // UNIT) % hops
    source = (row // CAP) % PAIR
    slot = row % CAP
    group = jnp.bitwise_xor(line, hop) * PAIR + jnp.bitwise_xor(core, half)
    here = source == core
    member = jnp.zeros((rows, count), jnp.bool_)
    weights = [jnp.zeros((rows, count), jnp.float32) for _ in range(EXP_DEV)]
    for name in range(names):
        expert = ids_ref[name : name + 1, :]
        value = route_ref[name : name + 1, :].astype(jnp.float32)
        for which in range(EXP_DEV):
            hit = expert == group * EXP_DEV + which
            member = member | hit
            weights[which] = weights[which] + jnp.where(hit, value, 0.0)
    member = member & here
    before = (
        lax.broadcasted_iota(jnp.int32, (count, count), 0)
        < lax.broadcasted_iota(jnp.int32, (count, count), 1)
    ).astype(jnp.bfloat16)
    order = jnp.dot(
        member.astype(jnp.float32).astype(jnp.bfloat16), before, preferred_element_type=jnp.float32
    )
    chosen = jnp.where(member & (order == slot.astype(jnp.float32)), 1.0, 0.0)
    place = chosen.astype(jnp.bfloat16)
    place_ref[...] = place
    lane = lax.broadcasted_iota(jnp.int32, (rows, LANES), 1)
    extra = jnp.zeros((rows, LANES), jnp.float32)
    for which in range(EXP_DEV):
        total = jnp.sum(chosen * weights[which], axis=1, keepdims=True)
        extra = extra + jnp.where(lane == which, total, 0.0)
    extra = extra.astype(jnp.bfloat16)
    keep_ref[:, width:] = extra[: rows // 2]
    give_ref[:, width:] = extra[rows // 2 :]

    def body(index, carry):
        start = pl.multiple_of(index * step, step)
        picked = jnp.dot(
            place, tokens_ref[:, pl.ds(start, step)], preferred_element_type=jnp.float32
        )
        pieces = []
        for block in range(step // QBLOCK):
            values = picked[:, block * QBLOCK : (block + 1) * QBLOCK]
            largest = jnp.max(jnp.abs(values), axis=1, keepdims=True)
            scale = ((largest + 1e-06) * (1.0 / 448.0)).astype(jnp.bfloat16).astype(jnp.float32)
            quantized = (values / scale).astype(jnp.bfloat16).astype(jnp.float32)
            pieces.append((quantized * scale).astype(jnp.bfloat16))
        result = jnp.concatenate(pieces, axis=1)
        keep_ref[:, pl.ds(start, step)] = result[: rows // 2]
        give_ref[:, pl.ds(start, step)] = result[rows // 2 :]
        return carry

    lax.fori_loop(0, width // step, body, 0)


def pack(where, ids, route, tokens, hops):
    count, width = tokens.shape
    rows = hops * UNIT
    step = 512 if width % 512 == 0 else QBLOCK
    sent = jax.ShapeDtypeStruct((rows, width + LANES), jnp.bfloat16)
    return pl.pallas_call(
        functools.partial(pack_kernel, hops, step),
        out_shape=(sent, sent, jax.ShapeDtypeStruct((2 * rows, count), jnp.bfloat16)),
        in_specs=[SMEM, VMEM, VMEM, VMEM],
        out_specs=(VMEM, VMEM, VMEM),
        compiler_params=pltpu.CompilerParams(vmem_limit_bytes=16 << 20),
        cost_estimate=pl.CostEstimate(
            flops=4 * rows * count * width, bytes_accessed=count * width * 4, transcendentals=0
        ),
        name="pack",
    )(where, ids, route, tokens)


def expert_kernel(counts, steps, chunk, *refs):
    n = len(counts)
    rows = refs[:n]
    gate_ref, up_ref, down_ref = refs[n : n + 3]
    outs = refs[n + 3 : 2 * n + 3]
    gathered, acc, hidden = refs[2 * n + 3 :]
    width = steps * chunk
    hid = gate_ref.shape[2]
    index = pl.program_id(0)

    @pl.when(index == 0)
    def _():
        offset = 0
        for ref, size in zip(rows, counts):
            gathered[offset : offset + size, :] = ref[...]
            offset += size
        acc[...] = jnp.zeros_like(acc)

    @pl.when(index < steps)
    def _():
        start = pl.multiple_of(index * chunk, chunk)
        block = gathered[:, pl.ds(start, chunk)]
        for expert in range(EXP_DEV):
            for side, ref in enumerate((gate_ref, up_ref)):
                at = (side * EXP_DEV + expert) * hid
                acc[:, at : at + hid] += jnp.dot(
                    block, ref[expert], preferred_element_type=jnp.float32
                )

    @pl.when(index == steps - 1)
    def _():
        for expert in range(EXP_DEV):
            gate = acc[:, expert * hid : (expert + 1) * hid]
            upper = acc[:, (EXP_DEV + expert) * hid : (EXP_DEV + expert + 1) * hid]
            weight = gathered[:, width + expert : width + expert + 1].astype(jnp.float32)
            value = gate / (1.0 + jnp.exp(-gate)) * upper * weight
            hidden[:, expert * hid : (expert + 1) * hid] = value.astype(jnp.bfloat16)

    @pl.when(index >= steps)
    def _():
        result = jnp.dot(hidden[...], down_ref[...], preferred_element_type=jnp.float32)
        result = result.astype(jnp.bfloat16)
        offset = 0
        for ref, size in zip(outs, counts):
            ref[...] = result[offset : offset + size]
            offset += size


def experts(pieces, w_gate, w_up, w_down):
    counts = tuple(piece.shape[0] for piece in pieces)
    total = sum(counts)
    width, hid = w_gate.shape[1], w_gate.shape[2]
    chunk = 512 if width % 512 == 0 else LANES
    steps = width // chunk
    down = w_down.reshape(EXP_DEV * hid, width)
    whole = [pl.BlockSpec(piece.shape, lambda i: (0, 0)) for piece in pieces]
    in_block = pl.BlockSpec((EXP_DEV, chunk, hid), lambda i: (0, jnp.minimum(i, steps - 1), 0))
    out_at = lambda i: (0, jnp.maximum(i - steps, 0))
    return pl.pallas_call(
        functools.partial(expert_kernel, counts, steps, chunk),
        grid=(2 * steps,),
        out_shape=[jax.ShapeDtypeStruct((size, width), jnp.bfloat16) for size in counts],
        in_specs=whole + [in_block, in_block, pl.BlockSpec((EXP_DEV * hid, chunk), out_at)],
        out_specs=[pl.BlockSpec((size, chunk), out_at) for size in counts],
        scratch_shapes=[
            pltpu.VMEM((total, width + LANES), jnp.bfloat16),
            pltpu.VMEM((total, 2 * EXP_DEV * hid), jnp.float32),
            pltpu.VMEM((total, EXP_DEV * hid), jnp.bfloat16),
        ],
        compiler_params=pltpu.CompilerParams(vmem_limit_bytes=32 << 20),
        cost_estimate=pl.CostEstimate(
            flops=6 * total * EXP_DEV * hid * width,
            bytes_accessed=6 * EXP_DEV * hid * width,
            transcendentals=total * EXP_DEV * hid,
        ),
        name="experts",
    )(*pieces, w_gate, w_up, down)


def unpack_kernel(place_ref, *refs):
    out_ref = refs[-1]
    rows = jnp.concatenate([ref[...] for ref in refs[:-1]], axis=0)
    out_ref[...] = lax.dot_general(
        place_ref[...], rows, (((0,), (0,)), ((), ())), preferred_element_type=jnp.float32
    ).astype(jnp.bfloat16)


def unpack(place, pieces):
    count = place.shape[1]
    width = pieces[0].shape[1]
    chunk = 1024 if width % 1024 == 0 else LANES
    return pl.pallas_call(
        unpack_kernel,
        grid=(width // chunk,),
        out_shape=jax.ShapeDtypeStruct((count, width), jnp.bfloat16),
        in_specs=[pl.BlockSpec(place.shape, lambda i: (0, 0))]
        + [pl.BlockSpec((piece.shape[0], chunk), lambda i: (0, i)) for piece in pieces],
        out_specs=pl.BlockSpec((count, chunk), lambda i: (0, i)),
        compiler_params=pltpu.CompilerParams(vmem_limit_bytes=16 << 20),
        cost_estimate=pl.CostEstimate(
            flops=2 * place.shape[0] * count * width,
            bytes_accessed=4 * count * width,
            transcendentals=0,
        ),
        name="unpack",
    )(place, *pieces)


def flip(value, axis, mask):
    size = lax.axis_size(axis)
    return lax.ppermute(value, axis, [(i, i ^ mask) for i in range(size)])


def shards(tokens, expert_ids, route_weight, w_gate, w_up, w_down):
    nodes = lax.axis_size("node")
    hops = lax.axis_size("torus") // PAIR
    spot = lax.axis_index("torus").astype(jnp.int32)
    where = jnp.stack([spot // PAIR, spot % PAIR])
    keep, give, place = pack(where, expert_ids.T, route_weight.T, tokens, hops)
    got = flip(give, "torus", 1)
    mine = [
        keep[hop * UNIT : (hop + 1) * UNIT] + got[hop * UNIT : (hop + 1) * UNIT]
        for hop in range(hops)
    ]
    landed = {0: mine[0]}
    for hop in range(1, hops):
        landed[hop] = flip(mine[hop], "torus", hop * PAIR)
    batches = [[0], list(range(1, hops - 1)), [hops - 1]]
    batches = [batch for batch in batches if batch]
    pieces = []
    for batch in batches:
        own = jnp.concatenate([landed[hop] for hop in batch], axis=0)
        pieces.append([own] + [flip(own, "node", mask) for mask in range(1, nodes)])
    flat = [piece for parts in pieces for piece in parts]
    results = experts(flat, w_gate, w_up, w_down)
    back = {}
    for number in reversed(range(len(batches))):
        parts = results[number * nodes : (number + 1) * nodes]
        total = parts[0].astype(jnp.float32)
        for mask in range(1, nodes):
            total = total + flip(parts[mask], "node", mask).astype(jnp.float32)
        total = total.astype(jnp.bfloat16)
        for place_in, hop in enumerate(batches[number]):
            part = total[place_in * UNIT : (place_in + 1) * UNIT]
            back[hop] = part if hop == 0 else flip(part, "torus", hop * PAIR)
    held = jnp.concatenate([back[hop] for hop in range(hops)], axis=0)
    other = flip(held, "torus", 1)
    return unpack(place, [held, other])


def solution(mesh):
    placed = (
        P(("node", "torus"), None),
        P(("node", "torus"), None),
        P(("node", "torus"), None),
        P("torus", None, "node"),
        P("torus", None, "node"),
        P("torus", "node", None),
    )
    return jax.shard_map(
        shards, mesh=mesh, in_specs=placed, out_specs=P(("node", "torus"), None), check_vma=False
    )
```

```python
import functools

import jax
import jax.numpy as jnp
from jax import lax
from jax.experimental import pallas as pl
from jax.experimental.pallas import tpu as pltpu
from jax.sharding import PartitionSpec as P


EXP_DEV = 2
CAP = 4
QBLOCK = 128
PAIR = 2
UNIT = PAIR * CAP
LANES = 128


VMEM = pl.BlockSpec(memory_space=pltpu.VMEM)
SMEM = pl.BlockSpec(memory_space=pltpu.SMEM)


def pack_kernel(hops, step, where_ref, ids_hbm, route_hbm, tokens_hbm, keep_ref, give_ref, place_ref, ids_ref, route_ref, tokens_ref, sems):
    count, width = tokens_ref.shape
    names = ids_ref.shape[0]
    chunks = width // step
    small = [
        pltpu.make_async_copy(ids_hbm, ids_ref, sems.at[chunks]),
        pltpu.make_async_copy(route_hbm, route_ref, sems.at[chunks + 1]),
    ]
    large = [
        pltpu.make_async_copy(
            tokens_hbm.at[:, pl.ds(index * step, step)],
            tokens_ref.at[:, pl.ds(index * step, step)],
            sems.at[index],
        )
        for index in range(chunks)
    ]
    for copy in small + large:
        copy.start()
    rows = 2 * hops * CAP
    line, core = where_ref[0], where_ref[1]
    row = lax.broadcasted_iota(jnp.int32, (rows, count), 0)
    half = row // (hops * CAP)
    hop = (row // CAP) % hops
    slot = row % CAP
    group = jnp.bitwise_xor(line, hop) * PAIR + jnp.bitwise_xor(core, half)
    before = (
        lax.broadcasted_iota(jnp.int32, (count, count), 0)
        < lax.broadcasted_iota(jnp.int32, (count, count), 1)
    ).astype(jnp.bfloat16)
    spread_row = lax.broadcasted_iota(jnp.int32, (PAIR * rows, rows), 0)
    spread_col = lax.broadcasted_iota(jnp.int32, (PAIR * rows, rows), 1)
    spread = (
        (spread_col == (spread_row // UNIT) * CAP + spread_row % CAP)
        & ((spread_row // CAP) % PAIR == core)
    ).astype(jnp.bfloat16)
    for copy in small:
        copy.wait()
    member = jnp.zeros((rows, count), jnp.bool_)
    weights = [jnp.zeros((rows, count), jnp.float32) for _ in range(EXP_DEV)]
    for name in range(names):
        expert = ids_ref[name : name + 1, :]
        value = route_ref[name : name + 1, :].astype(jnp.float32)
        for which in range(EXP_DEV):
            hit = expert == group * EXP_DEV + which
            member = member | hit
            weights[which] = weights[which] + jnp.where(hit, value, 0.0)
    order = jnp.dot(
        member.astype(jnp.float32).astype(jnp.bfloat16), before, preferred_element_type=jnp.float32
    )
    chosen = jnp.where(member & (order == slot.astype(jnp.float32)), 1.0, 0.0)
    place = chosen.astype(jnp.bfloat16)

    def spreading(value):
        return jnp.dot(spread, value, preferred_element_type=jnp.float32).astype(jnp.bfloat16)

    place_ref[...] = spreading(place)
    lane = lax.broadcasted_iota(jnp.int32, (rows, LANES), 1)
    extra = jnp.zeros((rows, LANES), jnp.float32)
    for which in range(EXP_DEV):
        total = jnp.sum(chosen * weights[which], axis=1, keepdims=True)
        extra = extra + jnp.where(lane == which, total, 0.0)
    extra = spreading(extra.astype(jnp.bfloat16))
    keep_ref[:, width:] = extra[:rows]
    give_ref[:, width:] = extra[rows:]
    for index in range(chunks):
        large[index].wait()
        span = slice(index * step, (index + 1) * step)
        picked = jnp.dot(place, tokens_ref[:, span], preferred_element_type=jnp.float32)
        pieces = []
        for block in range(step // QBLOCK):
            values = picked[:, block * QBLOCK : (block + 1) * QBLOCK]
            largest = jnp.max(jnp.abs(values), axis=1, keepdims=True)
            scale = ((largest + 1e-06) * (1.0 / 448.0)).astype(jnp.bfloat16).astype(jnp.float32)
            quantized = (values / scale).astype(jnp.bfloat16).astype(jnp.float32)
            pieces.append((quantized * scale).astype(jnp.bfloat16))
        result = spreading(jnp.concatenate(pieces, axis=1))
        keep_ref[:, span] = result[:rows]
        give_ref[:, span] = result[rows:]


def pack(where, ids, route, tokens, hops):
    count, width = tokens.shape
    rows = hops * UNIT
    step = width // 4 if width % (4 * QBLOCK) == 0 else width
    sent = jax.ShapeDtypeStruct((rows, width + LANES), jnp.bfloat16)
    hbm = pl.BlockSpec(memory_space=pltpu.HBM)
    held = [pltpu.with_memory_space_constraint(x, pltpu.HBM) for x in (ids, route, tokens)]
    return pl.pallas_call(
        functools.partial(pack_kernel, hops, step),
        out_shape=(sent, sent, jax.ShapeDtypeStruct((2 * rows, count), jnp.bfloat16)),
        in_specs=[SMEM, hbm, hbm, hbm],
        out_specs=(VMEM, VMEM, VMEM),
        scratch_shapes=[
            pltpu.VMEM(ids.shape, ids.dtype),
            pltpu.VMEM(route.shape, route.dtype),
            pltpu.VMEM(tokens.shape, tokens.dtype),
            pltpu.SemaphoreType.DMA((width // step + 2,)),
        ],
        compiler_params=pltpu.CompilerParams(vmem_limit_bytes=16 << 20),
        cost_estimate=pl.CostEstimate(
            flops=20 * 10**9, bytes_accessed=count * width * 4, transcendentals=0
        ),
        name="pack",
    )(where, *held)


def expert_kernel(counts, step, *refs):
    n = len(counts)
    rows = refs[:n]
    gate_ref, up_ref, down_ref = refs[n : n + 3]
    outs = refs[n + 3 : 2 * n + 3]
    gathered = refs[2 * n + 3]
    width = gate_ref.shape[1]
    offset = 0
    for ref, size in zip(rows, counts):
        gathered[offset : offset + size, :] = ref[...]
        offset += size
    block = gathered[:, :width]
    values = []
    for expert in range(EXP_DEV):
        gate = jnp.dot(block, gate_ref[expert], preferred_element_type=jnp.float32)
        upper = jnp.dot(block, up_ref[expert], preferred_element_type=jnp.float32)
        weight = gathered[:, width + expert : width + expert + 1].astype(jnp.float32)
        values.append((gate / (1.0 + jnp.exp(-gate)) * upper * weight).astype(jnp.bfloat16))
    hidden = jnp.concatenate(values, axis=1)

    def body(index, carry):
        start = pl.multiple_of(index * step, step)
        result = jnp.dot(
            hidden, down_ref[:, pl.ds(start, step)], preferred_element_type=jnp.float32
        ).astype(jnp.bfloat16)
        offset = 0
        for ref, size in zip(outs, counts):
            ref[:, pl.ds(start, step)] = result[offset : offset + size]
            offset += size
        return carry

    lax.fori_loop(0, width // step, body, 0)


def experts(pieces, w_gate, w_up, w_down):
    counts = tuple(piece.shape[0] for piece in pieces)
    total = sum(counts)
    width, hid = w_gate.shape[1], w_gate.shape[2]
    step = 1024 if width % 1024 == 0 else LANES
    down = w_down.reshape(EXP_DEV * hid, width)
    return pl.pallas_call(
        functools.partial(expert_kernel, counts, step),
        out_shape=[jax.ShapeDtypeStruct((size, width), jnp.bfloat16) for size in counts],
        in_specs=[VMEM] * (len(counts) + 3),
        out_specs=[VMEM] * len(counts),
        scratch_shapes=[pltpu.VMEM((total, width + LANES), jnp.bfloat16)],
        compiler_params=pltpu.CompilerParams(
            vmem_limit_bytes=(4 << 20) + 4 * total * (width + LANES)
        ),
        cost_estimate=pl.CostEstimate(
            flops=6 * total * EXP_DEV * hid * width,
            bytes_accessed=6 * EXP_DEV * hid * width,
            transcendentals=total * EXP_DEV * hid,
        ),
        name="experts",
    )(*pieces, w_gate, w_up, down)


def unpack_kernel(step, place_ref, *refs):
    rows, out_hbm, out_ref, sems = refs[:-3], refs[-3], refs[-2], refs[-1]
    width = out_ref.shape[1]
    place = place_ref[...].astype(jnp.float32).T.astype(jnp.bfloat16)
    copies = []
    for index in range(width // step):
        span = slice(index * step, (index + 1) * step)
        values = jnp.concatenate([ref[:, span] for ref in rows], axis=0)
        out_ref[:, span] = jnp.dot(place, values, preferred_element_type=jnp.float32).astype(
            jnp.bfloat16
        )
        copy = pltpu.make_async_copy(out_ref.at[:, span], out_hbm.at[:, span], sems.at[index])
        copy.start()
        copies.append(copy)
    for copy in copies:
        copy.wait()


def unpack(place, pieces):
    count = place.shape[1]
    width = pieces[0].shape[1]
    step = width // 4 if width % (4 * LANES) == 0 else width
    return pl.pallas_call(
        functools.partial(unpack_kernel, step),
        out_shape=jax.ShapeDtypeStruct((count, width), jnp.bfloat16),
        in_specs=[VMEM] * (1 + len(pieces)),
        out_specs=pl.BlockSpec(memory_space=pltpu.HBM),
        scratch_shapes=[
            pltpu.VMEM((count, width), jnp.bfloat16),
            pltpu.SemaphoreType.DMA((width // step,)),
        ],
        compiler_params=pltpu.CompilerParams(vmem_limit_bytes=16 << 20),
        cost_estimate=pl.CostEstimate(
            flops=2 * place.shape[0] * count * width,
            bytes_accessed=4 * count * width,
            transcendentals=0,
        ),
        name="unpack",
    )(place, *pieces)


def flip(value, axis, mask):
    size = lax.axis_size(axis)
    return lax.ppermute(value, axis, [(i, i ^ mask) for i in range(size)])


def plan(hops):
    batches = [[0], list(range(1, hops - 1)), [hops - 1]]
    return [batch for batch in batches if batch]


def shards(tokens, expert_ids, route_weight, w_gate, w_up, w_down):
    nodes = lax.axis_size("node")
    hops = lax.axis_size("torus") // PAIR
    spot = lax.axis_index("torus").astype(jnp.int32)
    where = jnp.stack([spot // PAIR, spot % PAIR])
    keep, give, place = pack(where, expert_ids.T, route_weight.T, tokens, hops)
    got = flip(give, "torus", 1)
    mine = [
        keep[hop * UNIT : (hop + 1) * UNIT] + got[hop * UNIT : (hop + 1) * UNIT]
        for hop in range(hops)
    ]
    landed = {0: mine[0]}
    for hop in range(1, hops):
        landed[hop] = flip(mine[hop], "torus", hop * PAIR)
    batches = plan(hops)
    flat = []
    for batch in batches:
        own = jnp.concatenate([landed[hop] for hop in batch], axis=0)
        flat.append(own)
        for mask in range(1, nodes):
            flat.append(flip(own, "node", mask))
    results = experts(flat, w_gate, w_up, w_down)
    back = {}
    for number in reversed(range(len(batches))):
        parts = results[number * nodes : (number + 1) * nodes]
        total = parts[0].astype(jnp.float32)
        for mask in range(1, nodes):
            received = flip(parts[mask], "node", mask)
            total = total + received.astype(jnp.float32)
        total = total.astype(jnp.bfloat16)
        for place_in, hop in enumerate(batches[number]):
            part = total[place_in * UNIT : (place_in + 1) * UNIT]
            back[hop] = part if hop == 0 else flip(part, "torus", hop * PAIR)
    held = jnp.concatenate([back[hop] for hop in range(hops)], axis=0)
    other = flip(held, "torus", 1)
    return unpack(place, [held, other])


def solution(mesh):
    placed = (
        P(("node", "torus"), None),
        P(("node", "torus"), None),
        P(("node", "torus"), None),
        P("torus", None, "node"),
        P("torus", None, "node"),
        P("torus", "node", None),
    )
    return jax.shard_map(
        shards, mesh=mesh, in_specs=placed, out_specs=P(("node", "torus"), None), check_vma=False
    )
```
